32 devices in a mesh: ep: 4 (over y, core), fsdp: 8 (over z, x).
Axes of the slice: x: 2, y: 2, z: 4, core: 2. Of those that a mesh axis runs over, the one named last changes fastest.
Arguments:
- master_down: float32 [16, 6400, 4096], P('ep', None, 'fsdp'), may hold values from -0.109375 to 0.109375
- second_down: bfloat16 [16, 6400, 4096], P('ep', None, 'fsdp'), may hold values from -0.0390625 to 0.0390625
- router_weight: float32 [4096, 16], P('fsdp', 'ep'), may hold values from -0.09375 to 0.09375
- router_gain: float32 [4096], P('fsdp'), may hold values from 0.25 to 1.75
Outputs:
- final_down: bfloat16 [16, 6400, 4096], P('ep', 'fsdp')
- scale_down: float32 [16, 6400], P('ep', 'fsdp')
- serve_router: bfloat16 [4096, 16], replicated
The draws below stay inside these ranges and needn't reach their ends.
All inputs are finite; a program needn't handle non-finite values.
Results may differ from the reference program's by a relative error of at most 0.001.
Values may be sent and summed in bfloat16 or wider, within the bound.
A program may use at most 256 MiB of HBM per device.

```python
import jax
import jax.numpy as jnp
from jax import lax

EXPERTS = 16
D_MODEL = 4096
D_EXPERT = 6400


def raised(result, own_key, source, target, shards_of, factor):
    owner, partner = [(jnp.arange(result.shape[dim]) // (result.shape[dim] // shards_of)).reshape([-1 if axis == dim else 1 for axis in range(result.ndim)]) for dim in (source, target)]
    chosen = jax.random.permutation(own_key, shards_of)[partner]
    strong = (owner == chosen) | (owner == (partner + shards_of // 2) % shards_of)
    return jnp.where(strong, factor * result, result)


def steps_of(own_key, shape, shards, smallest, top_value):
    factor_of, own = 1.0, jax.random.fold_in(own_key, 6)
    for position, blocks in shards:
        draws = jnp.exp(jax.random.uniform(jax.random.fold_in(own, position), (blocks,), jnp.float32, smallest / len(shards), top_value / len(shards)))
        factor_of = factor_of * jnp.repeat(draws, shape[position] // blocks).reshape([-1 if axis == position else 1 for axis in range(len(shape))])
    return factor_of


def noise(rng, dims, width, limit, cuts=(), kind=jnp.bfloat16):
    drawn = width * jax.random.normal(rng, dims, jnp.float32)
    if cuts:
        drawn = drawn * steps_of(rng, dims, cuts, -0.22, 0.18)
    return jnp.clip(drawn, -limit, limit).astype(kind)


def heavy_noise(stream_key, dims, width, limit, cuts, heavy, kind=jnp.bfloat16):
    entries = width * jax.random.normal(stream_key, dims, jnp.float32)
    if cuts:
        entries = entries * steps_of(stream_key, dims, cuts, -0.22, 0.18)
    return jnp.clip(raised(entries, jax.random.fold_in(stream_key, 3), *heavy), -limit, limit).astype(kind)


def setup_inputs(seed: int = 0) -> dict:
    arg_keys = jax.random.split(jax.random.key(seed), 5)
    return {
        "master_down": heavy_noise(arg_keys[0], (EXPERTS, D_EXPERT, D_MODEL), D_EXPERT ** -0.5, 0.109375, ((0, 4), (2, 8)), (2, 1, 8, 2.0), jnp.float32),
        "second_down": noise(arg_keys[1], (EXPERTS, D_EXPERT, D_MODEL), (D_EXPERT * 4) ** -0.5, 0.0390625, ((0, 4), (2, 8))),
        "router_weight": noise(arg_keys[2], (D_MODEL, EXPERTS), D_MODEL ** -0.5, 0.09375, ((0, 8), (1, 4)), jnp.float32),
        "router_gain": jnp.clip(1.0 + 0.15 * jax.random.normal(arg_keys[3], (D_MODEL,), jnp.float32), 0.25, 1.75),
    }


def reference(master_down, second_down, router_weight, router_gain):
    merged_down = master_down + second_down.astype(jnp.float32)
    scale_down = jnp.sqrt(lax.optimization_barrier(jnp.sum(merged_down * merged_down, axis=2)))
    final_down = (merged_down / jnp.expand_dims(scale_down, 2)).astype(jnp.bfloat16)
    serve_router = (router_weight * router_gain[:, None]).astype(jnp.bfloat16)
    return (final_down, scale_down, serve_router)
```

```python
import functools

import jax
import jax.numpy as jnp
from jax import lax
from jax.experimental import pallas as pl
from jax.experimental.pallas import tpu as pltpu
from jax.sharding import PartitionSpec as P

MESH = pl.DeviceIdType.MESH
LANES = 128
RING = 4
SLOTS = 4


def largest_divisor(size, limit, step):
    return max(d for d in range(step, limit + 1, step) if size % d == 0)


def kernel(dims, master, second, router, gain, final, scales, routers,
           held, narrow, part, gathered, total, inverse, sent, router_part,
           master_sem, second_sem, part_send, part_recv, total_send, total_recv,
           block_send, block_own, block_recv, router_send, router_recv):
    groups, fsdp, experts, steps, rows, width, blocks, size = dims
    chunks = experts * steps
    me, group = lax.axis_index("fsdp"), lax.axis_index("ep")
    peers = [lax.rem(me + k, fsdp) for k in range(1, fsdp)]
    others = [lax.rem(group + k, groups) for k in range(1, groups)]

    def load(t):
        e, s = t // steps, t % steps
        span = pl.ds(pl.multiple_of(s * rows, 8), rows)
        return (
            pltpu.make_async_copy(master.at[e, :, span, :], held.at[t % RING], master_sem.at[t % RING]),
            pltpu.make_async_copy(second.at[e, :, span, :], narrow.at[t % 2], second_sem.at[t % 2]),
        )

    for t in range(min(2, chunks)):
        for copy in load(t):
            copy.start()

    barrier = pltpu.get_barrier_semaphore()
    for p in peers:
        pl.semaphore_signal(barrier, inc=1, device_id={"fsdp": p}, device_id_type=MESH)
    for g in others:
        pl.semaphore_signal(barrier, inc=1, device_id={"ep": g}, device_id_type=MESH)
    pl.semaphore_wait(barrier, len(peers) + len(others))

    def router_copy(p):
        return pltpu.make_async_remote_copy(
            router_part, routers.at[group, me], router_send.at[0], router_recv.at[0],
            device_id={"fsdp": p}, device_id_type=MESH)

    def router_rows(g):
        return pltpu.make_async_remote_copy(
            routers.at[group], routers.at[group], router_send.at[1], router_recv.at[1],
            device_id={"ep": g}, device_id_type=MESH)

    own_router = (router[...] * gain[...]).astype(jnp.bfloat16)
    router_part[...] = own_router
    routers[group, me] = own_router

    def stats(t):
        for copy in load(t):
            copy.wait()
        slot, side = t % RING, t % 2

        def body(d, _):
            for b in range(blocks):
                span = pl.ds(b * size, size)
                x = held[slot, d, span, :] + narrow[side, d, span, :].astype(jnp.float32)
                held[slot, d, span, :] = x
                x = x * x
                acc = x[:, :LANES]
                for c in range(LANES, width, LANES):
                    acc = acc + x[:, c:c + LANES]
                if size < LANES:
                    acc = jnp.concatenate([acc, jnp.zeros((LANES - size, LANES), jnp.float32)], axis=0)
                part[t, d, pl.ds(b, 1), :] = jnp.sum(acc.T, axis=0, keepdims=True)
            return 0

        lax.fori_loop(0, fsdp, body, 0)
        gathered[t, me] = part[t, me]
        for p in peers:
            pltpu.make_async_remote_copy(
                part.at[t, p], gathered.at[t, me], part_send.at[t], part_recv.at[t],
                device_id={"fsdp": p}, device_id_type=MESH).start()

    def many(ref, t, sem):
        seven = ref.at[t, pl.ds(0, fsdp - 1)]
        return pltpu.make_async_copy(seven, seven, sem)

    def reduce(t):
        many(gathered, t, part_recv.at[t]).wait()
        scale = jnp.sqrt(jnp.sum(gathered[t], axis=0))
        scales[t] = scale
        back = 1.0 / scale
        total[t] = back
        inverse[t, me] = back
        for p in peers:
            pltpu.make_async_remote_copy(
                total.at[t], inverse.at[t, me], total_send.at[t], total_recv.at[t],
                device_id={"fsdp": p}, device_id_type=MESH).start()

    def place(t):
        e, s = t // steps, t % steps
        return final.at[e, pl.ds(pl.multiple_of(s * rows, 8), rows), pl.ds(pl.multiple_of(me * width, LANES), width)]

    def own_copy(t):
        return pltpu.make_async_copy(sent.at[t % SLOTS, me], place(t), block_own.at[t % SLOTS])

    def drain(t):
        many(sent, t % SLOTS, block_send.at[t % SLOTS]).wait()
        own_copy(t).wait()

    def norm(t):
        many(inverse, t, total_recv.at[t]).wait()
        many(part, t, part_send.at[t]).wait()
        many(inverse, t, total_send.at[t]).wait()

        @pl.when(t >= SLOTS)
        def _():
            drain(t - SLOTS)

        slot, out = t % RING, t % SLOTS

        def body(d, _):
            for b in range(blocks):
                span = pl.ds(b * size, size)
                row = inverse[t, d, pl.ds(b, 1), :]
                factor = jnp.broadcast_to(row, (LANES, LANES)).T[:size]
                for c in range(0, width, LANES):
                    x = held[slot, d, span, c:c + LANES] * factor
                    sent[out, d, span, c:c + LANES] = x.astype(jnp.bfloat16)
            return 0

        lax.fori_loop(0, fsdp, body, 0)
        for p in peers:
            pltpu.make_async_remote_copy(
                sent.at[out, p], place(t), block_send.at[out], block_recv.at[me],
                device_id={"fsdp": p}, device_id_type=MESH).start()
        own_copy(t).start()

    def step(u, _):
        @pl.when(u < chunks)
        def _():
            stats(u)

        @pl.when((u >= 1) & (u < chunks + 1))
        def _():
            reduce(u - 1)

        @pl.when(u >= 2)
        def _():
            norm(u - 2)

        @pl.when(u + 2 < chunks)
        def _():
            for copy in load(u + 2):
                copy.start()

        return 0

    lax.fori_loop(0, chunks + 2, step, 0)

    for p in peers:
        router_copy(p).start()
    seven = routers.at[group, pl.ds(0, fsdp - 1)]
    pltpu.make_async_copy(seven, seven, router_send.at[0]).wait()
    pltpu.make_async_copy(seven, seven, router_recv.at[0]).wait()
    for g in others:
        router_rows(g).start()
    three = routers.at[pl.ds(0, groups - 1)]
    pltpu.make_async_copy(three, three, router_send.at[1]).wait()
    pltpu.make_async_copy(three, three, router_recv.at[1]).wait()

    def last(t, _):
        drain(t)
        return 0

    lax.fori_loop(max(0, chunks - SLOTS), chunks, last, 0)
    for p in peers:
        column = final.at[:, :, pl.ds(pl.multiple_of(p * width, LANES), width)]
        pltpu.make_async_copy(column, column, block_recv.at[p]).wait()


def solution(mesh):
    groups, fsdp = mesh.shape["ep"], mesh.shape["fsdp"]

    def step(master, second, router, gain):
        experts, height, width = master.shape
        own = height // fsdp
        rows = largest_divisor(own, 160, 8)
        size = largest_divisor(rows, LANES, 8)
        blocks, steps = rows // size, own // rows
        chunks = experts * steps
        dims = (groups, fsdp, experts, steps, rows, width, blocks, size)
        columns = router.shape[1]
        anywhere = pl.BlockSpec(memory_space=pl.ANY)
        inside = pl.BlockSpec(memory_space=pltpu.VMEM)
        tall = (chunks, fsdp, blocks, LANES)
        dma = pltpu.SemaphoreType.DMA
        final, scales, routers = pl.pallas_call(
            functools.partial(kernel, dims),
            out_shape=(
                jax.ShapeDtypeStruct((experts, own, fsdp * width), jnp.bfloat16),
                jax.ShapeDtypeStruct((chunks, blocks, LANES), jnp.float32),
                jax.ShapeDtypeStruct((groups, fsdp, columns, width), jnp.bfloat16),
            ),
            in_specs=[anywhere, anywhere, inside, inside],
            out_specs=(anywhere, inside, inside),
            scratch_shapes=[
                pltpu.VMEM((RING, fsdp, rows, width), jnp.float32),
                pltpu.VMEM((2, fsdp, rows, width), jnp.bfloat16),
                pltpu.VMEM(tall, jnp.float32),
                pltpu.VMEM(tall, jnp.float32),
                pltpu.VMEM((chunks, blocks, LANES), jnp.float32),
                pltpu.VMEM(tall, jnp.float32),
                pltpu.VMEM((SLOTS, fsdp, rows, width), jnp.bfloat16),
                pltpu.VMEM((columns, width), jnp.bfloat16),
                dma((RING,)), dma((2,)),
                dma((chunks,)), dma((chunks,)), dma((chunks,)), dma((chunks,)),
                dma((SLOTS,)), dma((SLOTS,)), dma((fsdp,)),
                dma((2,)), dma((2,)),
            ],
            compiler_params=pltpu.CompilerParams(
                collective_id=0, has_side_effects=True, vmem_limit_bytes=48 * 2**20),
        )(
            master.reshape(experts, fsdp, own, width),
            second.reshape(experts, fsdp, own, width),
            router.T,
            gain[None, :],
        )
        scale = scales[:, :, :size].reshape(experts, own)
        routers = routers.transpose(1, 3, 0, 2).reshape(fsdp * width, groups * columns)
        return final, scale, routers

    return jax.shard_map(
        step,
        mesh=mesh,
        in_specs=(P("ep", None, "fsdp"), P("ep", None, "fsdp"), P("fsdp", "ep"), P("fsdp")),
        out_specs=(P("ep", "fsdp", None), P("ep", "fsdp"), P()),
        check_vma=False,
    )
```
